32 devices in a mesh: head: 4 (over y, core), seq: 8 (over z, x).
Axes of the slice: x: 2, y: 2, z: 4, core: 2. Of those that a mesh axis runs over, the one named last changes fastest.
Arguments:
- queries: bfloat16 [8192, 4096], P('seq', 'head'), may hold values from -6 to 6
- keys: bfloat16 [8192, 512], P('seq', 'head'), may hold values from -6 to 6
- values: bfloat16 [8192, 512], P('seq', 'head'), may hold values from -6 to 6
- vertical: int32 [32, 8], P('head'), may hold values from 0 to 63, as said below
- slash: int32 [32, 8], P('head'), may hold values from 1 to 28, as said below
Outputs:
- attended: bfloat16 [8192, 4096], P(('seq', 'head'))
The draws below stay inside these ranges and needn't reach their ends.
Inputs may be any that keep to these rules, and one draw needn't show every extreme that they name: `vertical`: each row names 8 different blocks. Within each group of 8 consecutive rows, the different blocks named that lie in one slab (blocks s * 8 to s * 8 + 7) number at most 4, and exactly 4 in some slab. `slash`: each row names 8 different offsets.
All inputs are finite; a program needn't handle non-finite values.
Results may differ from the reference program's by a relative error of at most 0.0033.
Values may be sent and summed in bfloat16 or wider, within the bound.
A program may use at most 128 MiB of HBM per device.

```python
import math
import jax
import jax.numpy as jnp
from jax import lax

HD = 128
QUERY_PER_GROUP = 8
BLK = 128
VERTICAL_BLOCKS = 8
SLASH_OFFSETS = 8
LARGEST_OFFSET = 28
CAP = 4
GROUPS = 4
HEADS = 32
BLK_DEV = 8
SLABS = 8
SEQ = 8192
BLOCKS = 64


def draw_queries(key, part):
    own_key = jax.random.fold_in(key, 11)
    drawn = jnp.clip(1.5 * jax.random.normal(own_key, (SEQ, GROUPS, QUERY_PER_GROUP, HD), jnp.float32), -6.0, 6.0)
    return drawn.reshape(SEQ, HEADS * HD).astype(jnp.bfloat16)


def draw_keys(key, part):
    own_key = jax.random.fold_in(key, 12)
    drawn = jnp.clip(1.5 * jax.random.normal(own_key, (SEQ, GROUPS, HD), jnp.float32), -6.0, 6.0)
    return drawn.reshape(SEQ, GROUPS * HD).astype(jnp.bfloat16)


def vertical_group(key):
    key_count, key_full, key_order, key_pick = jax.random.split(key, 4)
    slab_ids = jnp.arange(SLABS, dtype=jnp.int32)
    counts = jax.random.randint(key_count, (SLABS,), 1, CAP + 1)
    fullest = jax.random.randint(key_full, (), 0, SLABS)
    counts = jnp.where(slab_ids == fullest, CAP, counts)
    order_scores = jax.random.randint(key_order, (SLABS, BLK_DEV), 0, 4096) * BLK_DEV + jnp.arange(BLK_DEV, dtype=jnp.int32)[None, :]
    ranks = jnp.argsort(jnp.argsort(order_scores, axis=1), axis=1)
    inside = ranks < counts[:, None]
    mandatory_blocks = (inside & (slab_ids[:, None] == fullest)).reshape(BLOCKS)
    inside = inside.reshape(BLOCKS)
    selected_indices = jax.random.randint(key_pick, (QUERY_PER_GROUP, BLOCKS), 0, 65536) * BLOCKS + jnp.arange(BLOCKS, dtype=jnp.int32)[None, :] + 1
    selected_indices = jnp.where(inside[None, :], selected_indices, 0)
    extra_score = jnp.where((jnp.arange(QUERY_PER_GROUP)[:, None] == 0) & mandatory_blocks[None, :], 1 << 29, 0)
    leftover_slots, selected_blocks = lax.top_k(selected_indices + extra_score, VERTICAL_BLOCKS)
    return selected_blocks.astype(jnp.int32)


def draw_vertical(key, part):
    group_keys = jax.random.split(jax.random.fold_in(key, 31), GROUPS)
    return jax.vmap(vertical_group)(group_keys).reshape(HEADS, VERTICAL_BLOCKS).astype(jnp.int32)


def draw_slash(key, part):
    block_scores = jax.random.randint(jax.random.fold_in(key, 41), (HEADS, LARGEST_OFFSET), 0, 65536) * LARGEST_OFFSET + jnp.arange(LARGEST_OFFSET, dtype=jnp.int32)[None, :] + 1
    per_head_rows = jnp.arange(HEADS)[:, None]
    offset_columns = jnp.arange(LARGEST_OFFSET)[None, :]
    extra_score = jnp.where((per_head_rows == 0) & (offset_columns == LARGEST_OFFSET - 1), 1 << 28, 0)
    extra_score = extra_score + jnp.where((per_head_rows == 1) & (offset_columns == 0), 1 << 28, 0)
    leftover_slots, selected_blocks = lax.top_k(block_scores + extra_score, SLASH_OFFSETS)
    return (selected_blocks + 1).astype(jnp.int32)


def block_levels(key, extent, pieces, least, largest):
    factor_of, own = 1.0, jax.random.fold_in(key, 6)
    for position, shards_of in pieces:
        steps = jnp.exp(jax.random.uniform(jax.random.fold_in(own, position), (shards_of,), jnp.float32, least / len(pieces), largest / len(pieces)))
        factor_of = factor_of * jnp.repeat(steps, extent[position] // shards_of).reshape([-1 if axis == position else 1 for axis in range(len(extent))])
    return factor_of


def normal_values(rng, dims, scale, limit, cuts=(), held_as=jnp.bfloat16):
    level = block_levels(rng, dims, cuts, -0.22, 0.18) if cuts else 1.0
    values = jax.random.normal(rng, dims, jnp.float32) * scale * level
    return jnp.minimum(jnp.maximum(values, -limit), limit).astype(held_as)


def setup_inputs(seed: int = 0) -> dict:
    key_list = jax.random.split(jax.random.key(seed), 6)
    return {
        "queries": draw_queries(jax.random.fold_in(key_list[5], 71), 0),
        "keys": draw_keys(jax.random.fold_in(key_list[5], 71), 0),
        "values": normal_values(key_list[2], (SEQ, GROUPS * HD), 1.0, 6.0, ((0, 8), (1, 4))),
        "vertical": draw_vertical(jax.random.fold_in(key_list[5], 71), 0),
        "slash": draw_slash(jax.random.fold_in(key_list[5], 71), 0),
    }


NEG = -1e+30

def attend(query_block, diag_kv, slash_kv, column_kv, slash_ok, column_ok):
    block_count, block_width, head_width = query_block.shape
    slash_count = slash_kv.shape[1]
    column_count = column_kv.shape[0]
    score_scale = 1.0 / math.sqrt(head_width)
    causal = jnp.arange(block_width)[:, None] >= jnp.arange(block_width)[None, :]
    diag_scores = jnp.einsum('ird,icd->irc', query_block, diag_kv[..., :head_width]) * score_scale
    diag_scores = jnp.where(causal[None], diag_scores, NEG)
    slash_scores = jnp.einsum('ird,ijcd->irjc', query_block, slash_kv[..., :head_width]) * score_scale
    slash_scores = jnp.where(slash_ok[:, None, :, None], slash_scores, NEG).reshape(block_count, block_width, slash_count * block_width)
    column_scores = jnp.einsum('ird,jcd->irjc', query_block, column_kv[..., :head_width]) * score_scale
    column_scores = jnp.where(column_ok[:, None, :, None], column_scores, NEG).reshape(block_count, block_width, column_count * block_width)
    block_scores = jnp.concatenate([diag_scores, slash_scores, column_scores], axis=2)
    row_top = lax.optimization_barrier(jnp.max(block_scores, axis=2, keepdims=True))
    weights = jnp.exp(block_scores - row_top)
    row_total = lax.optimization_barrier(jnp.sum(weights, axis=2))
    rounded = lax.optimization_barrier(weights.astype(jnp.bfloat16)).astype(jnp.float32)
    split_one = block_width
    split_two = block_width + slash_count * block_width
    w_diag = rounded[:, :, :split_one]
    w_slash = rounded[:, :, split_one:split_two].reshape(block_count, block_width, slash_count, block_width)
    w_column = rounded[:, :, split_two:].reshape(block_count, block_width, column_count, block_width)
    mixed_sum = jnp.einsum('irc,icd->ird', w_diag, diag_kv[..., head_width:])
    mixed_sum = mixed_sum + jnp.einsum('irjc,ijcd->ird', w_slash, slash_kv[..., head_width:])
    mixed_sum = mixed_sum + jnp.einsum('irjc,jcd->ird', w_column, column_kv[..., head_width:])
    return (mixed_sum / row_total[:, :, None]).astype(jnp.bfloat16)

def reference(queries, keys, values, vertical, slash):
    seq_rows = queries.shape[0]
    block_total = seq_rows // BLK
    joined = jnp.concatenate([keys.reshape(seq_rows, GROUPS, HD), values.reshape(seq_rows, GROUPS, HD)], axis=2)
    block_ids = jnp.arange(block_total, dtype=jnp.int32)

    def one_head(head_index):
        group_index = head_index // QUERY_PER_GROUP
        query_block = lax.dynamic_slice_in_dim(queries, head_index * HD, HD, 1).astype(jnp.float32).reshape(block_total, BLK, HD)
        group_kv = lax.dynamic_index_in_dim(joined, group_index, 1, keepdims=False).astype(jnp.float32).reshape(block_total, BLK, 2 * HD)
        padded = jnp.concatenate([jnp.zeros((LARGEST_OFFSET, BLK, 2 * HD), jnp.float32), group_kv], axis=0)
        offsets = lax.dynamic_index_in_dim(slash, head_index, 0, keepdims=False)
        columns = lax.dynamic_index_in_dim(vertical, head_index, 0, keepdims=False)
        slash_index = (LARGEST_OFFSET + block_ids[:, None] - offsets[None, :]).astype(jnp.int32)
        slash_kv = jnp.take(padded, slash_index, axis=0)
        slash_ok = block_ids[:, None] - offsets[None, :] >= 0
        column_kv = jnp.take(group_kv, columns.astype(jnp.int32), axis=0)
        covered = jnp.any(block_ids[:, None, None] - columns[None, :, None] == offsets[None, None, :], axis=2)
        column_ok = (columns[None, :] < block_ids[:, None]) & jnp.logical_not(covered)
        return attend(query_block, group_kv, slash_kv, column_kv, slash_ok, column_ok)
    outputs = lax.map(one_head, jnp.arange(HEADS, dtype=jnp.int32))
    return jnp.transpose(outputs, (1, 2, 0, 3)).reshape(seq_rows, HEADS * HD)
```

```python
import functools
import math

import jax
import jax.numpy as jnp
from jax import lax
from jax.experimental import pallas as pl
from jax.experimental.pallas import tpu as pltpu
from jax.sharding import PartitionSpec as P

BLK = 128
LARGEST_OFFSET = 28
CAP = 4
NEG = -1e30
PIECES = 2
VALUE_STRIDE = 2
MIX_UNROLL = 4
RING = 8
VMEM_BYTES = 62 * 1024 * 1024
SPARE_BYTES = 3 * 1024 * 1024
MESH = pl.DeviceIdType.MESH


def half_columns(half):
    return slice(half * BLK, (half + 1) * BLK)


def beside(a, b):
    return jnp.concatenate([a, b], axis=1)


def stacked(a, b):
    return jnp.concatenate([a, b], axis=0)


def on_diagonal(a, b):
    zero = jnp.zeros((BLK, BLK), jnp.bfloat16)
    return stacked(beside(a, zero), beside(zero, b))


def layer_kernel(
    slash_ref,
    vertical_ref,
    queries_ref,
    keys_ref,
    values_ref,
    out_ref,
    index_ref,
    slash_bias,
    vertical_bias,
    rank_ref,
    used_ref,
    found_ref,
    pack_ref,
    q_ref,
    k_buf,
    v_buf,
    staged,
    weights,
    scores_even,
    scores_odd,
    top_even,
    top_odd,
    held,
    packed,
    held_sem,
    load_sem,
    chain_send,
    chain_recv,
    cross_send,
    cross_recv,
    out_local,
    out_send,
    out_recv,
    *,
    blocks,
    rounds,
    width,
    heads,
    slabs,
    groups,
):
    slab = lax.axis_index("seq")
    group = lax.axis_index("head")
    chain_len = slabs // 2
    place, side = slab // 2, slab % 2
    piece = blocks // PIECES
    bufs = (k_buf, v_buf)
    has_next = place + 1 < chain_len

    whole_blocks = slabs * blocks
    reach = (LARGEST_OFFSET + blocks - 1) // blocks
    pack_at = reach // 2
    cap_piece = CAP // PIECES

    def part(kv, place_of, side_of, c, far):
        origin = place_of * 2 + side_of
        if far:
            first = pl.multiple_of(whole_blocks + origin * CAP + c * cap_piece, cap_piece)
            return bufs[kv].at[pl.ds(first, cap_piece)]
        first = pl.multiple_of(origin * blocks + c * piece, piece)
        return bufs[kv].at[pl.ds(first, piece)]

    def sent(ref, t, kv, c, far):
        if t == pack_at and far:
            return packed.at[kv, pl.ds(c * cap_piece, cap_piece)]
        return ref

    def chain(t, kv, c):
        ref = part(kv, place - t, side, c, chain_far(t + 1))
        return pltpu.make_async_remote_copy(
            sent(ref, t, kv, c, chain_far(t + 1)), ref, chain_send.at[t, kv, c], chain_recv.at[t, kv, c],
            device_id={"seq": slab + 2}, device_id_type=MESH,
        )

    def chain_in(t, kv, c):
        ref = part(kv, place - t, side, c, chain_far(t))
        return pltpu.make_async_remote_copy(
            ref, ref, chain_send.at[t - 1, kv, c], chain_recv.at[t - 1, kv, c],
            device_id={"seq": slab - 2}, device_id_type=MESH,
        )

    def cross(t, kv, c, sender):
        ref = part(kv, place - t, sender, c, cross_far(t, sender))
        return pltpu.make_async_remote_copy(
            sent(ref, t, kv, c, cross_far(t, sender)), ref, cross_send.at[t, kv, c], cross_recv.at[t, kv, c],
            device_id={"seq": place * 2 + 1 - side}, device_id_type=MESH,
        )

    def chain_far(t):
        return 2 * t > reach

    def cross_far(t, sender):
        return (2 * t - 1 if sender else 2 * t + 1) > reach

    def cross_runs(t, sender, this_side):
        if t == 0 and sender == 1:
            return None
        return (side == this_side) & (place >= t)

    own_first = pl.multiple_of(slab * blocks, blocks)
    loads = [
        pltpu.make_async_copy(keys_ref, k_buf.at[pl.ds(own_first, blocks)], load_sem.at[0]),
        pltpu.make_async_copy(values_ref, held.at[1], load_sem.at[1]),
        pltpu.make_async_copy(queries_ref, q_ref, load_sem.at[2]),
    ]
    for load in loads:
        load.start()

    barrier = pltpu.get_barrier_semaphore()
    pl.semaphore_signal(
        barrier, 1, device_id={"seq": place * 2 + 1 - side}, device_id_type=MESH
    )
    for d in range(1, groups):
        pl.semaphore_signal(
            barrier, 1, device_id={"head": lax.rem(group + d, groups)}, device_id_type=MESH
        )

    @pl.when(has_next)
    def _():
        pl.semaphore_signal(barrier, 1, device_id={"seq": slab + 2}, device_id_type=MESH)

    @pl.when(place > 0)
    def _():
        pl.semaphore_signal(barrier, 1, device_id={"seq": slab - 2}, device_id_type=MESH)

    pl.semaphore_wait(
        barrier, groups + has_next.astype(jnp.int32) + (place > 0).astype(jnp.int32)
    )
    def start_cross(t, kv, c, packed):
        for sender in range(2):
            runs = cross_runs(t, sender, sender)
            if runs is not None and (t == pack_at and cross_far(t, sender)) == packed:

                @pl.when(runs)
                def _():
                    cross(t, kv, c, sender).start()

    def start_chain(t, kv, c, packed):
        if t < chain_len - 1 and (t == pack_at and chain_far(t + 1)) == packed:

            @pl.when((place >= t) & has_next)
            def _():
                chain(t, kv, c).start()

    def pass_on(t, kv, c):
        if t > 0:

            @pl.when(place >= t)
            def _():
                chain_in(t, kv, c).wait_recv()

        start_chain(t, kv, c, False)
        start_cross(t, kv, c, False)
        if t == pack_at and c == PIECES - 1:

            @pl.when(place >= t)
            def _():
                first = pl.multiple_of(((place - t) * 2 + side) * blocks, blocks)
                move = pltpu.make_async_copy(
                    bufs[kv].at[pl.ds(first, blocks)], held.at[kv], held_sem.at[kv]
                )
                move.start()
                move.wait()
                for k in range(CAP):
                    packed[kv, k] = held[kv, pack_ref[k]]

            for each in range(PIECES):
                start_chain(t, kv, each, True)
                start_cross(t, kv, each, True)

    def wait_cross(kv):
        for t in range(chain_len):
            for c in range(PIECES):
                for sender in range(2):
                    runs = cross_runs(t, sender, 1 - sender)
                    if runs is not None:

                        @pl.when(runs)
                        def _():
                            cross(t, kv, c, sender).wait_recv()

    base = slab * blocks
    slashes, verticals = slash_ref.shape[1], vertical_ref.shape[1]

    def rank_block(block, rank):
        used = block < 0
        for head in range(heads):
            for n in range(verticals):
                used = used | (vertical_ref[head, n] == block)
        rank = jnp.where(block % blocks == 0, 0, rank)
        rank_ref[block] = rank
        used_ref[block] = used.astype(jnp.int32)
        return rank + used.astype(jnp.int32)

    def place_verticals(head, carry):
        for n in range(verticals):
            block = vertical_ref[head, n]
            far = whole_blocks + (block // blocks) * CAP + rank_ref[block]
            found = jnp.where(block >= (slab - reach) * blocks, block, far)
            found_ref[head * verticals + n] = jnp.where(block < base + blocks, found, base)
        return carry

    def list_blocks(step, carry):
        head, own = step // blocks, base + step % blocks
        reached = [own - slash_ref[head, n] for n in range(slashes)]
        for n, block in enumerate(reached):
            ok = block >= 0
            index_ref[step * slashes + n] = jnp.where(ok, block, own)
            slash_bias[step * slashes + n] = jnp.where(ok, 0.0, NEG)
        for n in range(verticals):
            block = vertical_ref[head, n]
            ok = block < own
            for other in reached:
                ok = ok & (block != other)
            vertical_bias[step * verticals + n] = jnp.where(ok, 0.0, NEG)
        return carry

    lists = heads * blocks
    loads[0].wait()
    for c in range(PIECES):
        pass_on(0, 0, c)
    lax.fori_loop(0, whole_blocks, rank_block, jnp.int32(0))
    packed_first = jnp.maximum((place - pack_at) * 2 + side, 0) * blocks
    for k in range(CAP):
        at = jnp.int32(0)
        for n in range(blocks):
            block = packed_first + n
            hit = (used_ref[block] == 1) & (rank_ref[block] == k)
            at = at + jnp.where(hit, n, 0)
        pack_ref[k] = at
    loads[1].wait()
    for n in range(blocks):
        v_buf[own_first + n] = held[1, n].T
    for t in range(1, chain_len):
        for c in range(PIECES):
            pass_on(t, 0, c)
        if t == 1:
            lax.fori_loop(0, heads, place_verticals, 0)
            lax.fori_loop(0, lists // 4, list_blocks, 0)
        if t == 2:
            lax.fori_loop(lists // 4, lists // 2, list_blocks, 0)
    for c in range(PIECES):
        pass_on(0, 1, c)
    lax.fori_loop(lists // 2, lists, list_blocks, 0)
    wait_cross(0)
    loads[2].wait()

    factor = math.log2(math.e) / math.sqrt(width)
    causal = lax.broadcasted_iota(jnp.int32, (BLK, BLK), 0) <= lax.broadcasted_iota(
        jnp.int32, (BLK, BLK), 1
    )
    share = blocks // groups
    share_rows = share * BLK

    def out_columns(group_of, head):
        return pl.ds(pl.multiple_of((group_of * heads + head) * width, width), width)

    def owner_of(r):
        return (group // 2 + r // 2 + 1) % (groups // 2) * 2 + (group + r + 1) % 2

    def sender_of(r):
        return (group // 2 + groups // 2 - 1 - r // 2) % (groups // 2) * 2 + (group + r + 1) % 2

    def out_copy(head, r):
        owner = owner_of(r)
        return pltpu.make_async_remote_copy(
            staged.at[head, pl.ds(pl.multiple_of(owner * share_rows, share_rows), share_rows)],
            out_ref.at[:, out_columns(group, head)],
            out_send.at[head, r], out_recv.at[head, r],
            device_id={"head": owner}, device_id_type=MESH,
        )

    def out_in(head, r):
        sender = sender_of(r)
        return pltpu.make_async_remote_copy(
            staged.at[head, pl.ds(0, share_rows)],
            out_ref.at[:, out_columns(sender, head)],
            out_send.at[head, r], out_recv.at[head, r],
            device_id={"head": sender}, device_id_type=MESH,
        )

    def out_own(head):
        return pltpu.make_async_copy(
            staged.at[head, pl.ds(pl.multiple_of(group * share_rows, share_rows), share_rows)],
            out_ref.at[:, out_columns(group, head)],
            out_local.at[head],
        )

    listed = 1 + slashes + verticals
    pairs = heads * blocks // 2 // rounds
    pairs_of_share = share // 2
    chunk_count = slashes // 2 + 1
    live = slab >= 0
    values_due = []
    for t in range(1, chain_len):
        each = [[(t, c)] for c in range(PIECES)]
        values_due += [sum(each, [])] if t == pack_at else each

    def pair_of(pair):
        r, rest = pair // (heads * pairs_of_share), pair % (heads * pairs_of_share)
        return r, rest // pairs_of_share, owner_of(r) * share + rest % pairs_of_share * 2

    def listed_pair(buf, pair, n):
        r, head, i = pair_of(pair)
        if n == 0:
            return buf[base + i], buf[base + i + 1]
        if n <= slashes:
            row = (head * blocks + i) * slashes + n - 1
            return buf[index_ref[row]], buf[index_ref[row + slashes]]
        shared = buf[found_ref[head * verticals + n - 1 - slashes]]
        return shared, shared

    def bias_of(pair, n, half):
        r, head, i = pair_of(pair)
        step = head * blocks + i + half
        if n <= slashes:
            return slash_bias[step * slashes + n - 1]
        return vertical_bias[step * verticals + n - 1 - slashes]

    chunks = []
    for c in range(chunk_count):
        near = [0] if c == 0 else [2 * c - 1, 2 * c]
        chunks.append((near, [1 + slashes + n for n in range(2 * c, min(2 * c + 2, verticals))]))

    def weigh_round(first, *accs):
        ring = (accs[:RING], accs[RING:])
        buffers = ((scores_even, top_even), (scores_odd, top_odd))

        def members(c):
            for j in range(2):
                for m in range(2):
                    if j < len(chunks[c][m]):
                        slot = 2 * c + j if m else max(2 * c - 1, 0) + j
                        yield m, chunks[c][m][j], ring[m][slot if slot < RING else 1]

        def stage(pair):
            r, head, i = pair_of(first + pair)
            columns = pl.ds(pl.multiple_of(head * width, width), width)
            both = [
                q_ref[pl.ds(pl.multiple_of((i + u) * BLK, BLK), BLK), columns] for u in range(2)
            ]
            pltpu.matmul_push_rhs(on_diagonal(*both), 0, 0, transpose=True)
            scaled = []
            for q in both:
                exact = q.astype(jnp.float32) * factor
                high = exact.astype(jnp.bfloat16)
                scaled.append(beside(high, (exact - high.astype(jnp.float32)).astype(jnp.bfloat16)))
            pltpu.matmul_push_rhs(stacked(*scaled), 0, 1, transpose=True)

        def score(pair, c):
            fresh = [c == 0, c == 0]
            for m, n, acc in members(c):
                pltpu.matmul_acc_lhs(
                    acc, beside(*listed_pair(k_buf, first + pair, n)), load_staged_rhs=0 if fresh[m] else None
                )
                fresh[m] = False

        def take(pair, c, scores, top):
            tops = [None, None]
            for m, n, acc in members(c):
                both = pltpu.matmul_pop(acc)
                for half in range(2):
                    x = both[:, half_columns(half)]
                    if n == 0:
                        x = jnp.where(causal, x, NEG)
                    scores[n * BLK : (n + 1) * BLK, half_columns(half)] = x
                    x = jnp.max(x.reshape(BLK // 8, 8, BLK), axis=0)
                    if n > 0:
                        x = x + bias_of(first + pair, n, half)
                    if m == 0:
                        x = x * factor
                    tops[half] = x if tops[half] is None else jnp.maximum(tops[half], x)
            for half in range(2):
                x = tops[half]
                if c > 0:
                    x = jnp.maximum(x, top[:, half_columns(half)])
                if c == chunk_count - 1:
                    x = jnp.broadcast_to(jnp.max(x, axis=0, keepdims=True), (8, BLK))
                top[:, half_columns(half)] = x

        def weigh(pair, c, scores, top):
            for m, n, _ in members(c):
                for half in range(2):
                    x = scores[n * BLK : (n + 1) * BLK, half_columns(half)]
                    shift = top[0:1, half_columns(half)]
                    if n > 0:
                        shift = shift - bias_of(first + pair, n, half)
                    if m == 0:
                        x = x * factor
                    weights[pair, n * BLK : (n + 1) * BLK, half_columns(half)] = jnp.exp2(
                        x - shift
                    ).astype(jnp.bfloat16)

        def one_pair(step, parity):
            now = step
            last, older = jnp.maximum(step - 1, 0), jnp.maximum(step - 2, 0)
            mine, other = buffers[parity], buffers[1 - parity]

            def part(c):
                if c == 0:
                    score(now, 0)
                    take(last, chunk_count - 2, *other)
                    weigh(older, chunk_count - 2, *mine)
                elif c == 1:
                    take(last, chunk_count - 1, *other)
                    score(now, 1)
                    weigh(older, chunk_count - 1, *mine)
                else:
                    score(now, c)
                    if c == chunk_count - 1:
                        stage(jnp.minimum(step + 1, pairs - 1))
                    take(now, c - 2, *mine)
                    weigh(last, c - 2, *other)

            for c in range(chunk_count):
                pl.when(live)(functools.partial(part, c))

        for m in range(2):
            for acc in ring[m]:
                pltpu.matmul_pop(acc)
        stage(0)

        def two_pairs(step, carry):
            if first == 0:
                for k, due in enumerate(values_due):

                    @pl.when(step == min(VALUE_STRIDE * (k + 1), pairs // 2 - 1))
                    def _():
                        for t, c in due:
                            pass_on(t, 1, c)

            one_pair(2 * step, 0)
            one_pair(2 * step + 1, 1)
            return carry

        lax.fori_loop(0, pairs // 2, two_pairs, 0)
        for c in range(chunk_count - 2, chunk_count):
            take(pairs - 1, c, *buffers[1])
            weigh(pairs - 2, c, *buffers[0])
        for c in range(chunk_count):
            weigh(pairs - 1, c, *buffers[1])
        for m in range(2):
            pltpu.matmul_acc_lhs(
                ring[m][0], jnp.zeros((BLK, 2 * BLK), jnp.bfloat16), load_staged_rhs=0
            )
            pltpu.matmul_pop(ring[m][0])

    def mix_round(first, *accs):
        ones = jnp.ones((16, 2 * BLK), jnp.bfloat16)

        def mix(pair, m, acc):
            slot = 0
            for n in range(1 + slashes):
                w = weights[pair, n * BLK : (n + 1) * BLK, :]
                pltpu.matmul_push_rhs(on_diagonal(w[:, :BLK], w[:, BLK:]), slot, m)
                lhs = beside(*listed_pair(v_buf, first + pair, n))
                pltpu.matmul_acc_lhs(acc, stacked(lhs, ones), load_staged_rhs=slot)
                slot = 1 - slot
                yield
            for n in range(1 + slashes, listed, 2):
                pltpu.matmul_push_rhs(weights[pair, n * BLK : (n + 2) * BLK, :], slot, m)
                lhs = beside(*[listed_pair(v_buf, first + pair, n + u)[0] for u in range(2)])
                pltpu.matmul_acc_lhs(acc, stacked(lhs, ones), load_staged_rhs=slot)
                slot = 1 - slot
                yield

        def some_pairs(step, carry):
            at = step * 2 * MIX_UNROLL
            for u in range(MIX_UNROLL):
                for _ in zip(
                    mix(at + 2 * u, 0, accs[u]), mix(at + 2 * u + 1, 1, accs[MIX_UNROLL + u])
                ):
                    pass
            for u in range(MIX_UNROLL):
                for m in range(2):
                    r, head, i = pair_of(first + at + 2 * u + m)
                    mixed = pltpu.matmul_pop(accs[m * MIX_UNROLL + u])
                    for half in range(2):
                        out = mixed[:width, half_columns(half)] / mixed[width : width + 1, half_columns(half)]
                        rows = pl.ds(pl.multiple_of((i + half) * BLK, BLK), BLK)
                        staged[head, rows, :] = out.T.astype(jnp.bfloat16)
            for u in range(2 * MIX_UNROLL // pairs_of_share):
                r, head, i = pair_of(first + at + u * pairs_of_share)

                @pl.when(r < groups - 1)
                def _():
                    out_copy(head, r).start()

                @pl.when(r == groups - 1)
                def _():
                    out_own(head).start()

            return carry

        for acc in accs:
            pltpu.matmul_pop(acc)
        lax.fori_loop(0, pairs // (2 * MIX_UNROLL), some_pairs, 0)

    for each in range(rounds):
        pl.run_scoped(
            functools.partial(weigh_round, each * pairs),
            *[pltpu.ACC(m)((BLK, 2 * BLK), jnp.float32) for m in range(2) for _ in range(RING)],
        )
        if each == 0:
            wait_cross(1)
        pl.run_scoped(
            functools.partial(mix_round, each * pairs),
            *[pltpu.ACC(m)((width + 16, 2 * BLK), jnp.float32) for m in range(2) for _ in range(MIX_UNROLL)],
        )

    for kv in range(2):
        for t in range(chain_len):
            for c in range(PIECES):
                if t < chain_len - 1:

                    @pl.when((place >= t) & has_next)
                    def _():
                        chain(t, kv, c).wait_send()

                for sender in range(2):
                    runs = cross_runs(t, sender, sender)
                    if runs is not None:

                        @pl.when(runs)
                        def _():
                            cross(t, kv, c, sender).wait_send()

    def finish(head, carry):
        out_own(head).wait()
        for r in range(groups - 1):
            out_copy(head, r).wait_send()
            out_in(head, r).wait_recv()
        return carry

    lax.fori_loop(0, heads, finish, 0)


def shards(queries, keys, values, vertical, slash):
    width = keys.shape[1]
    rows = queries.shape[0]
    blocks = rows // BLK
    heads = vertical.shape[0]
    slabs, groups = lax.axis_size("seq"), lax.axis_size("head")
    k = keys.reshape(blocks, BLK, width)
    v = values.reshape(blocks, BLK, width)
    slashes, verticals = slash.shape[1], vertical.shape[1]
    listed = 1 + slashes + verticals
    pairs = heads * blocks // 2
    room = VMEM_BYTES - 4 * (2 * BLK * width * slabs * (blocks + CAP) // 2)
    room -= 4 * rows * heads * width + 2 * 4 * listed * BLK * 2 * BLK + SPARE_BYTES
    rounds = 1
    while pairs // rounds * listed * BLK * 2 * BLK * 2 > room:
        rounds *= 2
    dma = pltpu.SemaphoreType.DMA
    hops = (slabs // 2, 2, PIECES)
    smem, anywhere = pl.BlockSpec(memory_space=pltpu.SMEM), pl.BlockSpec(memory_space=pl.ANY)
    return pl.pallas_call(
        functools.partial(
            layer_kernel,
            blocks=blocks,
            rounds=rounds,
            width=width,
            heads=heads,
            slabs=slabs,
            groups=groups,
        ),
        in_specs=[smem, smem, anywhere, anywhere, anywhere],
        out_specs=anywhere,
        out_shape=jax.ShapeDtypeStruct((rows // groups, groups * heads * width), jnp.bfloat16),
        scratch_shapes=[
            pltpu.SMEM((heads * blocks * slashes,), jnp.int32),
            pltpu.SMEM((heads * blocks * slashes,), jnp.float32),
            pltpu.SMEM((heads * blocks * verticals,), jnp.float32),
            pltpu.SMEM((slabs * blocks,), jnp.int32),
            pltpu.SMEM((slabs * blocks,), jnp.int32),
            pltpu.SMEM((vertical.size,), jnp.int32),
            pltpu.SMEM((CAP,), jnp.int32),
            pltpu.VMEM(queries.shape, jnp.bfloat16),
            pltpu.VMEM((slabs * (blocks + CAP), BLK, width), jnp.bfloat16),
            pltpu.VMEM((slabs * (blocks + CAP), width, BLK), jnp.bfloat16),
            pltpu.VMEM((heads, rows, width), jnp.bfloat16),
            pltpu.VMEM((pairs // rounds, listed * BLK, 2 * BLK), jnp.bfloat16),
            pltpu.VMEM((listed * BLK, 2 * BLK), jnp.float32),
            pltpu.VMEM((listed * BLK, 2 * BLK), jnp.float32),
            pltpu.VMEM((8, 2 * BLK), jnp.float32),
            pltpu.VMEM((8, 2 * BLK), jnp.float32),
            pltpu.VMEM((2, blocks, BLK, width), jnp.bfloat16),
            pltpu.VMEM((2, CAP, BLK, width), jnp.bfloat16),
            dma((2,)),
            dma((3,)),
            dma(hops),
            dma(hops),
            dma(hops),
            dma(hops),
            dma((heads,)),
            dma((heads, groups - 1)),
            dma((heads, groups - 1)),
        ],
        compiler_params=pltpu.CompilerParams(
            collective_id=0, has_side_effects=True, vmem_limit_bytes=VMEM_BYTES
        ),
    )(slash, vertical, queries, k, v)


def solution(mesh):
    in_specs = (
        P("seq", "head"),
        P("seq", "head"),
        P("seq", "head"),
        P("head", None),
        P("head", None),
    )
    out_specs = P(("seq", "head"), None)
    return jax.shard_map(shards, mesh=mesh, in_specs=in_specs, out_specs=out_specs, check_vma=False)
```

```python
import functools
import itertools
import math

import jax
import jax.numpy as jnp
from jax import lax
from jax.experimental import pallas as pl
from jax.experimental.pallas import tpu as pltpu
from jax.sharding import PartitionSpec as P

BLK = 128
LARGEST_OFFSET = 28
CAP = 4
NEG = -1e30
PIECES = 2
VALUE_STEPS = (3, 7, 8, 9, 12)
MIX_UNROLL = 4
GATED = True
RING = 8
VMEM_BYTES = 62 * 1024 * 1024
SPARE_BYTES = 3 * 1024 * 1024
MESH = pl.DeviceIdType.MESH


def half_columns(half):
    return slice(half * BLK, (half + 1) * BLK)


def beside(a, b):
    return jnp.concatenate([a, b], axis=1)


def stacked(a, b):
    return jnp.concatenate([a, b], axis=0)


def on_diagonal(a, b):
    zero = jnp.zeros((BLK, BLK), jnp.bfloat16)
    return stacked(beside(a, zero), beside(zero, b))


def layer_kernel(
    slash_ref,
    vertical_ref,
    queries_ref,
    keys_ref,
    values_ref,
    out_ref,
    named_ref,
    offsets_ref,
    found_ref,
    pack_ref,
    own_pack_ref,
    block_ref,
    bias_even,
    bias_odd,
    q_ref,
    k_buf,
    v_buf,
    staged,
    weights,
    scores_even,
    scores_odd,
    top_even,
    top_odd,
    held,
    packed,
    packed_own,
    turn_sem,
    held_sem,
    load_sem,
    chain_send,
    chain_recv,
    cross_send,
    cross_recv,
    out_local,
    out_send,
    out_recv,
    *,
    blocks,
    rounds,
    width,
    heads,
    slabs,
    groups,
):
    slab = lax.axis_index("seq")
    group = lax.axis_index("head")
    chain_len = slabs // 2
    place, side = slab // 2, slab % 2
    piece = blocks // PIECES
    bufs = (k_buf, v_buf)
    has_next = place + 1 < chain_len

    whole_blocks = slabs * blocks
    reach = (LARGEST_OFFSET + blocks - 1) // blocks
    pack_at = reach // 2
    cap_piece = CAP // PIECES
    jump = pack_at + 1
    has_far = place + jump < chain_len

    def part(kv, place_of, side_of, c, far):
        origin = place_of * 2 + side_of
        if far:
            first = pl.multiple_of(whole_blocks + origin * CAP + c * cap_piece, cap_piece)
            return bufs[kv].at[pl.ds(first, cap_piece)]
        first = pl.multiple_of(origin * blocks + c * piece, piece)
        return bufs[kv].at[pl.ds(first, piece)]

    def sent(ref, t, kv, c, far):
        if t == pack_at and far:
            return packed.at[kv, pl.ds(c * cap_piece, cap_piece)]
        return ref

    def chain(t, kv, c):
        ref = part(kv, place - t, side, c, chain_far(t + 1))
        return pltpu.make_async_remote_copy(
            sent(ref, t, kv, c, chain_far(t + 1)), ref, chain_send.at[t, kv, c], chain_recv.at[t, kv, c],
            device_id={"seq": slab + 2}, device_id_type=MESH,
        )

    def direct(kv, c):
        ref = part(kv, place, side, c, True)
        return pltpu.make_async_remote_copy(
            packed_own.at[kv, pl.ds(c * cap_piece, cap_piece)], ref,
            chain_send.at[pack_at, kv, c], chain_recv.at[pack_at, kv, c],
            device_id={"seq": slab + 2 * jump}, device_id_type=MESH,
        )

    def start_direct(kv):
        for k in range(CAP):
            block = held[kv, own_pack_ref[k]]
            packed_own[kv, k] = block.T if kv else block

        for c in range(PIECES):

            @pl.when(has_far)
            def _():
                direct(kv, c).start()

    def chain_in(t, kv, c):
        ref = part(kv, place - t, side, c, chain_far(t))
        return pltpu.make_async_remote_copy(
            ref, ref, chain_send.at[t - 1, kv, c], chain_recv.at[t - 1, kv, c],
            device_id={"seq": slab - 2}, device_id_type=MESH,
        )

    def cross(t, kv, c, sender):
        ref = part(kv, place - t, sender, c, cross_far(t, sender))
        return pltpu.make_async_remote_copy(
            sent(ref, t, kv, c, cross_far(t, sender)), ref, cross_send.at[t, kv, c], cross_recv.at[t, kv, c],
            device_id={"seq": place * 2 + 1 - side}, device_id_type=MESH,
        )

    def chain_far(t):
        return 2 * t > reach

    def cross_far(t, sender):
        return (2 * t - 1 if sender else 2 * t + 1) > reach

    def cross_runs(t, sender, this_side):
        if t == 0 and sender == 1:
            return None
        return (side == this_side) & (place >= t)

    own_first = pl.multiple_of(slab * blocks, blocks)
    loads = [
        pltpu.make_async_copy(keys_ref, k_buf.at[pl.ds(own_first, blocks)], load_sem.at[0]),
        pltpu.make_async_copy(values_ref, held.at[1], load_sem.at[1]),
        pltpu.make_async_copy(queries_ref, q_ref, load_sem.at[2]),
        pltpu.make_async_copy(keys_ref, held.at[0], load_sem.at[3]),
    ]
    for load in loads:
        load.start()

    barrier = pltpu.get_barrier_semaphore()
    pl.semaphore_signal(
        barrier, 1, device_id={"seq": place * 2 + 1 - side}, device_id_type=MESH
    )
    for d in range(1, groups):
        pl.semaphore_signal(
            barrier, 1, device_id={"head": lax.rem(group + d, groups)}, device_id_type=MESH
        )

    @pl.when(has_next)
    def _():
        pl.semaphore_signal(barrier, 1, device_id={"seq": slab + 2}, device_id_type=MESH)

    @pl.when(place > 0)
    def _():
        pl.semaphore_signal(barrier, 1, device_id={"seq": slab - 2}, device_id_type=MESH)

    @pl.when(has_far)
    def _():
        pl.semaphore_signal(
            barrier, 1, device_id={"seq": slab + 2 * jump}, device_id_type=MESH
        )

    @pl.when(place >= jump)
    def _():
        pl.semaphore_signal(
            barrier, 1, device_id={"seq": slab - 2 * jump}, device_id_type=MESH
        )

    pl.semaphore_wait(
        barrier,
        groups
        + has_next.astype(jnp.int32)
        + (place > 0).astype(jnp.int32)
        + has_far.astype(jnp.int32)
        + (place >= jump).astype(jnp.int32),
    )
    def start_cross(t, kv, c, packed):
        for sender in range(2):
            runs = cross_runs(t, sender, sender)
            if runs is not None and (t == pack_at and cross_far(t, sender)) == packed:

                @pl.when(runs)
                def _():
                    cross(t, kv, c, sender).start()

    def chain_runs(t):
        if t == pack_at:
            return has_far
        return (place >= t) & has_next

    def chain_of(t, kv, c):
        return direct(kv, c) if t == pack_at else chain(t, kv, c)

    def start_chain(t, kv, c):
        if t < chain_len - 1 and t != pack_at:

            @pl.when(chain_runs(t))
            def _():
                chain(t, kv, c).start()

    def arrive(t, kv, c):
        @pl.when(place >= t)
        def _():
            chain_in(t, kv, c).wait_recv()

    def pack_arrived(kv):
        t = pack_at

        @pl.when(place >= t)
        def _():
            first = pl.multiple_of(((place - t) * 2 + side) * blocks, blocks)
            move = pltpu.make_async_copy(
                bufs[kv].at[pl.ds(first, blocks)], held.at[kv], held_sem.at[kv]
            )
            move.start()
            move.wait()
            for k in range(CAP):
                packed[kv, k] = held[kv, pack_ref[k]]

        for each in range(PIECES):
            start_cross(t, kv, each, True)

    def pass_on(t, kv, c):
        arrive(t, kv, c)
        start_chain(t, kv, c)
        start_cross(t, kv, c, False)
        if t == pack_at and c == PIECES - 1:
            pack_arrived(kv)

    order = [t for t in range(1, chain_len) if t != pack_at]
    order.insert(min(2, len(order)), pack_at)

    def wait_cross(kv):
        for t in range(chain_len):
            for c in range(PIECES):
                for sender in range(2):
                    runs = cross_runs(t, sender, 1 - sender)
                    if runs is not None:

                        @pl.when(runs)
                        def _():
                            cross(t, kv, c, sender).wait_recv()

    base = slab * blocks
    slashes, verticals = slash_ref.shape[1], vertical_ref.shape[1]

    low = blocks.bit_length() - 1

    def names(head, words):
        for n in range(verticals):
            block = vertical_ref[head, n]
            bit = jnp.int32(1) << (block & 31)
            words = tuple(
                word | jnp.where((block >> 5) == w, bit, 0) for w, word in enumerate(words)
            )
        offsets = jnp.int32(0)
        for n in range(slashes):
            offsets = offsets | (jnp.int32(1) << slash_ref[head, n])
        offsets_ref[head] = offsets
        return words

    def place_verticals(head, carry):
        for n in range(verticals):
            block = vertical_ref[head, n]
            first = (block >> low) << low
            in_slab = named_ref[block >> 5] >> (first & 31)
            below = in_slab & ((jnp.int32(1) << (block - first)) - 1)
            rank = jnp.int32(0)
            for u in range(blocks - 1):
                rank = rank + ((below >> u) & 1)
            found = jnp.where(
                block >= (slab - reach) * blocks, block, whole_blocks + (block >> low) * CAP + rank
            )
            found_ref[head * verticals + n] = jnp.where(block < base + blocks, found, base)
        return carry

    def list_pack(to_ref, of_slab):
        first = of_slab * blocks
        in_slab = named_ref[first >> 5] >> (first & 31)
        at = [jnp.int32(0) for _ in range(CAP)]
        count = jnp.int32(0)
        for n in range(blocks):
            hit = (in_slab >> n) & 1
            at = [x + jnp.where((hit == 1) & (count == k), n, 0) for k, x in enumerate(at)]
            count = count + hit
        for k in range(CAP):
            to_ref[k] = at[k]

    second = group % 2
    partner = group + 1 - 2 * second
    loads[0].wait()

    @pl.when(second == 0)
    def _():
        for c in range(PIECES):
            start_chain(0, 0, c)
            start_cross(0, 0, c, False)

    words = tuple(jnp.int32(0) for _ in range((whole_blocks + 31) // 32))
    for w, word in enumerate(lax.fori_loop(0, heads, names, words)):
        named_ref[w] = word
    list_pack(own_pack_ref, slab)
    loads[3].wait()
    loads[1].wait()

    @pl.when(second == 1)
    def _():
        if GATED:
            pl.semaphore_wait(turn_sem, 1)
        for c in range(PIECES):
            start_chain(0, 0, c)
            start_cross(0, 0, c, False)

    start_direct(0)
    list_pack(pack_ref, jnp.maximum((place - pack_at) * 2 + side, 0))
    for t in order:
        for c in range(PIECES):
            pass_on(t, 0, c)
        if t == 1:
            if GATED:

                @pl.when(second == 0)
                def _():
                    for sent_t in range(min(2, chain_len - 1)):
                        for c in range(PIECES):

                            @pl.when(chain_runs(sent_t))
                            def _():
                                chain_of(sent_t, 0, c).wait_send()

                    pl.semaphore_signal(
                        turn_sem, 1, device_id={"head": partner}, device_id_type=MESH
                    )

            lax.fori_loop(0, heads, place_verticals, 0)
            for n in range(blocks):
                v_buf[own_first + n] = held[1, n].T
    wait_cross(0)
    loads[2].wait()

    factor = math.log2(math.e) / math.sqrt(width)
    causal = lax.broadcasted_iota(jnp.int32, (BLK, BLK), 0) <= lax.broadcasted_iota(
        jnp.int32, (BLK, BLK), 1
    )
    share = blocks // groups
    share_rows = share * BLK

    def out_columns(group_of, head):
        return pl.ds(pl.multiple_of((group_of * heads + head) * width, width), width)

    def owner_of(r):
        return (group // 2 + r // 2 + 1) % (groups // 2) * 2 + (group + r + 1) % 2

    def sender_of(r):
        return (group // 2 + groups // 2 - 1 - r // 2) % (groups // 2) * 2 + (group + r + 1) % 2

    def out_copy(head, r):
        owner = owner_of(r)
        return pltpu.make_async_remote_copy(
            staged.at[head, pl.ds(pl.multiple_of(owner * share_rows, share_rows), share_rows)],
            out_ref.at[:, out_columns(group, head)],
            out_send.at[head, r], out_recv.at[head, r],
            device_id={"head": owner}, device_id_type=MESH,
        )

    def out_in(head, r):
        sender = sender_of(r)
        return pltpu.make_async_remote_copy(
            staged.at[head, pl.ds(0, share_rows)],
            out_ref.at[:, out_columns(sender, head)],
            out_send.at[head, r], out_recv.at[head, r],
            device_id={"head": sender}, device_id_type=MESH,
        )

    def out_own(head):
        return pltpu.make_async_copy(
            staged.at[head, pl.ds(pl.multiple_of(group * share_rows, share_rows), share_rows)],
            out_ref.at[:, out_columns(group, head)],
            out_local.at[head],
        )

    listed = 1 + slashes + verticals
    pairs = heads * blocks // 2 // rounds
    pairs_of_share = share // 2
    chunk_count = slashes // 2 + 1
    values_due = [[(0, c) for c in range(PIECES)]]
    for t in order:
        each = [[(t, c)] for c in range(PIECES)]
        values_due += [sum(each, [])] if t >= pack_at else each

    for q in range(blocks // 2):
        block_ref[q] = owner_of(q // pairs_of_share) * share + q % pairs_of_share * 2

    def pair_of(pair):
        q = lax.div(pair, heads)
        return lax.rem(pair, heads), q, block_ref[q]

    def reached(head, own, n):
        return own - slash_ref[head, n - 1]

    def listed_pair(buf, head, i, n):
        if n == 0:
            return buf[base + i], buf[base + i + 1]
        if n <= slashes:
            both = [reached(head, base + i + half, n) for half in range(2)]
            return [buf[jnp.where(x >= 0, x, base + i + half)] for half, x in enumerate(both)]
        shared = buf[found_ref[head * verticals + n - 1 - slashes]]
        return shared, shared

    def bias_of(head, i, n, half):
        own = base + i + half
        if n <= slashes:
            return jnp.where(reached(head, own, n) >= 0, 0.0, NEG)
        back = own - vertical_ref[head, n - 1 - slashes]
        covered = (offsets_ref[head] >> jnp.clip(back, 0, 31)) & 1
        return jnp.where((back > 0) & (covered == 0), 0.0, NEG)

    chunks = []
    for c in range(chunk_count):
        near = [0] if c == 0 else [2 * c - 1, 2 * c]
        chunks.append((near, [1 + slashes + n for n in range(2 * c, min(2 * c + 2, verticals))]))

    def weigh_round(first, *accs):
        ring = (accs[:RING], accs[RING:])
        buffers = (
            (scores_even, top_even, bias_even), (scores_odd, top_odd, bias_odd)
        )

        def members(c):
            for j in range(2):
                for m in range(2):
                    if j < len(chunks[c][m]):
                        slot = 2 * c + j if m else max(2 * c - 1, 0) + j
                        yield m, chunks[c][m][j], ring[m][slot if slot < RING else 1]

        def stage(head, i):
            columns = pl.ds(pl.multiple_of(head * width, width), width)
            both = [
                q_ref[pl.ds(pl.multiple_of((i + u) * BLK, BLK), BLK), columns] for u in range(2)
            ]
            pltpu.matmul_push_rhs(on_diagonal(*both), 0, 0, transpose=True)
            scaled = []
            for q in both:
                exact = q.astype(jnp.float32) * factor
                high = exact.astype(jnp.bfloat16)
                scaled.append(beside(high, (exact - high.astype(jnp.float32)).astype(jnp.bfloat16)))
            pltpu.matmul_push_rhs(stacked(*scaled), 0, 1, transpose=True)

        def score(head, i, c):
            fresh = [c == 0, c == 0]
            for m, n, acc in members(c):
                pltpu.matmul_acc_lhs(
                    acc, beside(*listed_pair(k_buf, head, i, n)), load_staged_rhs=0 if fresh[m] else None
                )
                fresh[m] = False

        def take(head, i, c, scores, top, biases):
            tops = [None, None]
            for m, n, acc in members(c):
                both = pltpu.matmul_pop(acc)
                for half in range(2):
                    x = both[:, half_columns(half)]
                    if n == 0:
                        x = jnp.where(causal, x, NEG)
                    scores[n * BLK : (n + 1) * BLK, half_columns(half)] = x
                    x = jnp.max(x.reshape(BLK // 8, 8, BLK), axis=0)
                    if n > 0:
                        bias = bias_of(head, i, n, half)
                        biases[2 * n + half] = bias
                        x = x + bias
                    if m == 0:
                        x = x * factor
                    tops[half] = x if tops[half] is None else jnp.maximum(tops[half], x)
                    yield
            for half in range(2):
                x = tops[half]
                if c > 0:
                    x = jnp.maximum(x, top[:, half_columns(half)])
                if c == chunk_count - 1:
                    x = jnp.broadcast_to(jnp.max(x, axis=0, keepdims=True), (8, BLK))
                top[:, half_columns(half)] = x

        def weigh(slot, c, scores, top, biases):
            for m, n, _ in members(c):
                for half in range(2):
                    x = scores[n * BLK : (n + 1) * BLK, half_columns(half)]
                    shift = top[0:1, half_columns(half)]
                    if n > 0:
                        shift = shift - biases[2 * n + half]
                    if m == 0:
                        x = x * factor
                    weights[slot, half, n * BLK : (n + 1) * BLK, :] = jnp.exp2(
                        x - shift
                    ).astype(jnp.bfloat16)
                    yield

        def drain(*steps):
            for step in steps:
                for _ in step:
                    pass

        def alternate(a, b):
            for _ in itertools.zip_longest(a, b):
                pass

        def advance(head, q):
            wraps = head + 1 == heads
            q = jnp.minimum(q + wraps.astype(jnp.int32), blocks // 2 - 1)
            return jnp.where(wraps, 0, head + 1), q, block_ref[q]

        def one_pair(step, parity, head, q, i, last_head, last_i):
            last, older = jnp.maximum(step - 1, 0), jnp.maximum(step - 2, 0)
            mine, other = buffers[parity], buffers[1 - parity]
            next_head, next_q, next_i = advance(head, q)

            def part(c):
                if c == 1:
                    alternate(
                        weigh(older, chunk_count - 1, *mine),
                        take(last_head, last_i, chunk_count - 1, *other),
                    )
                    score(head, i, 1)
                    return
                score(head, i, c)
                if c == 0:
                    alternate(
                        weigh(older, chunk_count - 2, *mine),
                        take(last_head, last_i, chunk_count - 2, *other),
                    )
                    return
                if c == chunk_count - 1:
                    stage(next_head, next_i)
                alternate(weigh(last, c - 2, *other), take(head, i, c - 2, *mine))

            for c in range(chunk_count):
                pl.when(slab > -1 - c // 2)(functools.partial(part, c))
            return next_head, next_q, next_i, head, i

        for m in range(2):
            for acc in ring[m]:
                pltpu.matmul_pop(acc)
        begin = pair_of(jnp.int32(first))
        stage(begin[0], begin[2])

        def two_pairs(step, carry):
            if first == 0:
                for k, due in enumerate(values_due):

                    @pl.when(step == min(VALUE_STEPS[min(k, len(VALUE_STEPS) - 1)], pairs // 2 - 1))
                    def _():
                        for t, c in due:
                            if t == 0:
                                start_cross(0, 1, c, False)
                                start_chain(0, 1, c)
                            else:
                                pass_on(t, 1, c)
                        if k == 0:
                            start_direct(1)

            carry = one_pair(2 * step, 0, *carry)
            return one_pair(2 * step + 1, 1, *carry)

        carry = lax.fori_loop(0, pairs // 2, two_pairs, (*begin, begin[0], begin[2]))
        for c in range(chunk_count - 2, chunk_count):
            drain(take(*carry[3:], c, *buffers[1]), weigh(pairs - 2, c, *buffers[0]))
        for c in range(chunk_count):
            drain(weigh(pairs - 1, c, *buffers[1]))
        for m in range(2):
            pltpu.matmul_acc_lhs(
                ring[m][0], jnp.zeros((BLK, 2 * BLK), jnp.bfloat16), load_staged_rhs=0
            )
            pltpu.matmul_pop(ring[m][0])

    def mix_round(first, *accs):
        ones = jnp.ones((16, 2 * BLK), jnp.bfloat16)

        def mix(pair, m, acc):
            head, _, i = pair_of(first + pair)
            slot = 0
            for n in range(1 + slashes):
                both = [weights[pair, half, n * BLK : (n + 1) * BLK, :] for half in range(2)]
                pltpu.matmul_push_rhs(on_diagonal(*both), slot, m)
                lhs = beside(*listed_pair(v_buf, head, i, n))
                pltpu.matmul_acc_lhs(acc, stacked(lhs, ones), load_staged_rhs=slot)
                slot = 1 - slot
                yield
            for n in range(1 + slashes, listed, 2):
                both = [weights[pair, half, n * BLK : (n + 2) * BLK, :] for half in range(2)]
                pltpu.matmul_push_rhs(beside(*both), slot, m)
                lhs = beside(*[listed_pair(v_buf, head, i, n + u)[0] for u in range(2)])
                pltpu.matmul_acc_lhs(acc, stacked(lhs, ones), load_staged_rhs=slot)
                slot = 1 - slot
                yield

        def some_pairs(step, carry):
            at = step * 2 * MIX_UNROLL
            for u in range(MIX_UNROLL):
                for _ in zip(
                    mix(at + 2 * u, 0, accs[u]), mix(at + 2 * u + 1, 1, accs[MIX_UNROLL + u])
                ):
                    pass
            for u in range(MIX_UNROLL):
                for m in range(2):
                    head, _, i = pair_of(first + at + 2 * u + m)
                    mixed = pltpu.matmul_pop(accs[m * MIX_UNROLL + u])
                    for half in range(2):
                        out = mixed[:width, half_columns(half)] / mixed[width : width + 1, half_columns(half)]
                        rows = pl.ds(pl.multiple_of((i + half) * BLK, BLK), BLK)
                        staged[head, rows, :] = out.T.astype(jnp.bfloat16)
            for u in range(2 * MIX_UNROLL):
                head, q, _ = pair_of(first + at + u)
                r = lax.div(q, pairs_of_share)
                whole = lax.rem(q, pairs_of_share) == pairs_of_share - 1

                @pl.when(whole & (r < groups - 1))
                def _():
                    out_copy(head, r).start()

                @pl.when(whole & (r == groups - 1))
                def _():
                    out_own(head).start()

            return carry

        for acc in accs:
            pltpu.matmul_pop(acc)
        lax.fori_loop(0, pairs // (2 * MIX_UNROLL), some_pairs, 0)

    for each in range(rounds):
        pl.run_scoped(
            functools.partial(weigh_round, each * pairs),
            *[pltpu.ACC(m)((BLK, 2 * BLK), jnp.float32) for m in range(2) for _ in range(RING)],
        )
        if each == 0:
            wait_cross(1)
        pl.run_scoped(
            functools.partial(mix_round, each * pairs),
            *[pltpu.ACC(m)((width + 16, 2 * BLK), jnp.float32) for m in range(2) for _ in range(MIX_UNROLL)],
        )

    for kv in range(2):
        for t in range(chain_len):
            for c in range(PIECES):
                if t < chain_len - 1:

                    runs = chain_runs(t)
                    if GATED and t < 2 and kv == 0:
                        runs = runs & (second == 1)

                    @pl.when(runs)
                    def _():
                        chain_of(t, kv, c).wait_send()

                for sender in range(2):
                    runs = cross_runs(t, sender, sender)
                    if runs is not None:

                        @pl.when(runs)
                        def _():
                            cross(t, kv, c, sender).wait_send()

    def finish(head, carry):
        out_own(head).wait()
        for r in range(groups - 1):
            out_copy(head, r).wait_send()
            out_in(head, r).wait_recv()
        return carry

    lax.fori_loop(0, heads, finish, 0)


def shards(queries, keys, values, vertical, slash):
    width = keys.shape[1]
    rows = queries.shape[0]
    blocks = rows // BLK
    heads = vertical.shape[0]
    slabs, groups = lax.axis_size("seq"), lax.axis_size("head")
    k = keys.reshape(blocks, BLK, width)
    v = values.reshape(blocks, BLK, width)
    slashes, verticals = slash.shape[1], vertical.shape[1]
    listed = 1 + slashes + verticals
    pairs = heads * blocks // 2
    room = VMEM_BYTES - 4 * (2 * BLK * width * slabs * (blocks + CAP) // 2)
    room -= 4 * rows * heads * width + 2 * 4 * listed * BLK * 2 * BLK + SPARE_BYTES
    rounds = 1
    while pairs // rounds * listed * BLK * 2 * BLK * 2 > room:
        rounds *= 2
    dma = pltpu.SemaphoreType.DMA
    hops = (slabs // 2, 2, PIECES)
    smem, anywhere = pl.BlockSpec(memory_space=pltpu.SMEM), pl.BlockSpec(memory_space=pl.ANY)
    return pl.pallas_call(
        functools.partial(
            layer_kernel,
            blocks=blocks,
            rounds=rounds,
            width=width,
            heads=heads,
            slabs=slabs,
            groups=groups,
        ),
        in_specs=[smem, smem, anywhere, anywhere, anywhere],
        out_specs=anywhere,
        out_shape=jax.ShapeDtypeStruct((rows // groups, groups * heads * width), jnp.bfloat16),
        scratch_shapes=[
            pltpu.SMEM(((slabs * blocks + 31) // 32,), jnp.int32),
            pltpu.SMEM((heads,), jnp.int32),
            pltpu.SMEM((vertical.size,), jnp.int32),
            pltpu.SMEM((CAP,), jnp.int32),
            pltpu.SMEM((CAP,), jnp.int32),
            pltpu.SMEM((blocks // 2,), jnp.int32),
            pltpu.SMEM((2 * listed,), jnp.float32),
            pltpu.SMEM((2 * listed,), jnp.float32),
            pltpu.VMEM(queries.shape, jnp.bfloat16),
            pltpu.VMEM((slabs * (blocks + CAP), BLK, width), jnp.bfloat16),
            pltpu.VMEM((slabs * (blocks + CAP), width, BLK), jnp.bfloat16),
            pltpu.VMEM((heads, rows, width), jnp.bfloat16),
            pltpu.VMEM((pairs // rounds, 2, listed * BLK, BLK), jnp.bfloat16),
            pltpu.VMEM((listed * BLK, 2 * BLK), jnp.float32),
            pltpu.VMEM((listed * BLK, 2 * BLK), jnp.float32),
            pltpu.VMEM((8, 2 * BLK), jnp.float32),
            pltpu.VMEM((8, 2 * BLK), jnp.float32),
            pltpu.VMEM((2, blocks, BLK, width), jnp.bfloat16),
            pltpu.VMEM((2, CAP, BLK, width), jnp.bfloat16),
            pltpu.VMEM((2, CAP, BLK, width), jnp.bfloat16),
            pltpu.SemaphoreType.REGULAR,
            dma((2,)),
            dma((4,)),
            dma(hops),
            dma(hops),
            dma(hops),
            dma(hops),
            dma((heads,)),
            dma((heads, groups - 1)),
            dma((heads, groups - 1)),
        ],
        compiler_params=pltpu.CompilerParams(
            collective_id=0, has_side_effects=True, vmem_limit_bytes=VMEM_BYTES
        ),
    )(slash, vertical, queries, k, v)


def solution(mesh):
    in_specs = (
        P("seq", "head"),
        P("seq", "head"),
        P("seq", "head"),
        P("head", None),
        P("head", None),
    )
    out_specs = P(("seq", "head"), None)
    return jax.shard_map(shards, mesh=mesh, in_specs=in_specs, out_specs=out_specs, check_vma=False)
```

```python
import functools
import itertools
import math

import jax
import jax.numpy as jnp
from jax import lax
from jax.experimental import pallas as pl
from jax.experimental.pallas import tpu as pltpu
from jax.sharding import PartitionSpec as P

BLK = 128
LARGEST_OFFSET = 28
CAP = 4
NEG = -1e30
PIECES = 2
FIRST_STEPS = (1, 1, 3, 4)
SECOND_STEPS = (3, 7)
MIX_UNROLL = 2
ROUNDS = 2
RING = 8
VMEM_BYTES = 62 * 1024 * 1024
SPARE_BYTES = 3 * 1024 * 1024
MESH = pl.DeviceIdType.MESH


def half_columns(half):
    return slice(half * BLK, (half + 1) * BLK)


def beside(a, b):
    return jnp.concatenate([a, b], axis=1)


def stacked(a, b):
    return jnp.concatenate([a, b], axis=0)


def on_diagonal(a, b):
    zero = jnp.zeros((BLK, BLK), jnp.bfloat16)
    return stacked(beside(a, zero), beside(zero, b))


def layer_kernel(
    slash_ref,
    vertical_ref,
    queries_ref,
    keys_ref,
    values_ref,
    out_ref,
    named_ref,
    offsets_ref,
    found_ref,
    pack_ref,
    own_pack_ref,
    block_ref,
    bias_even,
    bias_odd,
    q_ref,
    k_buf,
    v_buf,
    staged,
    weights,
    scores_even,
    scores_odd,
    top_even,
    top_odd,
    held,
    packed,
    packed_own,
    turn_sem,
    held_sem,
    load_sem,
    chain_send,
    chain_recv,
    cross_send,
    cross_recv,
    out_local,
    out_send,
    out_recv,
    *,
    blocks,
    rounds,
    width,
    heads,
    slabs,
    groups,
):
    slab = lax.axis_index("seq")
    group = lax.axis_index("head")
    chain_len = slabs // 2
    place, side = slab // 2, slab % 2
    piece = blocks // PIECES
    bufs = (k_buf, v_buf)
    has_next = place + 1 < chain_len

    whole_blocks = slabs * blocks
    reach = (LARGEST_OFFSET + blocks - 1) // blocks
    pack_at = reach // 2
    cap_piece = CAP // PIECES
    jump = pack_at + 1
    has_far = place + jump < chain_len

    def part(kv, place_of, side_of, c, far):
        origin = place_of * 2 + side_of
        if far:
            first = pl.multiple_of(whole_blocks + origin * CAP + c * cap_piece, cap_piece)
            return bufs[kv].at[pl.ds(first, cap_piece)]
        first = pl.multiple_of(origin * blocks + c * piece, piece)
        return bufs[kv].at[pl.ds(first, piece)]

    def sent(ref, t, kv, c, far):
        if t == pack_at and far:
            return packed.at[kv, pl.ds(c * cap_piece, cap_piece)]
        return ref

    def chain(t, kv, c):
        ref = part(kv, place - t, side, c, chain_far(t + 1))
        return pltpu.make_async_remote_copy(
            sent(ref, t, kv, c, chain_far(t + 1)), ref, chain_send.at[t, kv, c], chain_recv.at[t, kv, c],
            device_id={"seq": slab + 2}, device_id_type=MESH,
        )

    def direct(kv, c):
        ref = part(kv, place, side, c, True)
        return pltpu.make_async_remote_copy(
            packed_own.at[kv, pl.ds(c * cap_piece, cap_piece)], ref,
            chain_send.at[pack_at, kv, c], chain_recv.at[pack_at, kv, c],
            device_id={"seq": slab + 2 * jump}, device_id_type=MESH,
        )

    def start_direct(kv):
        for k in range(CAP):
            block = held[kv, own_pack_ref[k]]
            packed_own[kv, k] = block.T if kv else block

        for c in range(PIECES):

            @pl.when(has_far)
            def _():
                direct(kv, c).start()

    def chain_in(t, kv, c):
        ref = part(kv, place - t, side, c, chain_far(t))
        return pltpu.make_async_remote_copy(
            ref, ref, chain_send.at[t - 1, kv, c], chain_recv.at[t - 1, kv, c],
            device_id={"seq": slab - 2}, device_id_type=MESH,
        )

    def cross(t, kv, c, sender):
        ref = part(kv, place - t, sender, c, cross_far(t, sender))
        return pltpu.make_async_remote_copy(
            sent(ref, t, kv, c, cross_far(t, sender)), ref, cross_send.at[t, kv, c], cross_recv.at[t, kv, c],
            device_id={"seq": place * 2 + 1 - side}, device_id_type=MESH,
        )

    def chain_far(t):
        return 2 * t > reach

    def cross_far(t, sender):
        return (2 * t - 1 if sender else 2 * t + 1) > reach

    def cross_runs(t, sender, this_side):
        if t == 0 and sender == 1:
            return None
        return (side == this_side) & (place >= t)

    own_first = pl.multiple_of(slab * blocks, blocks)
    loads = [
        pltpu.make_async_copy(keys_ref, k_buf.at[pl.ds(own_first, blocks)], load_sem.at[0]),
        pltpu.make_async_copy(values_ref, held.at[1], load_sem.at[1]),
        pltpu.make_async_copy(queries_ref, q_ref, load_sem.at[2]),
        pltpu.make_async_copy(keys_ref, held.at[0], load_sem.at[3]),
    ]
    for load in loads:
        load.start()

    barrier = pltpu.get_barrier_semaphore()
    pl.semaphore_signal(
        barrier, 1, device_id={"seq": place * 2 + 1 - side}, device_id_type=MESH
    )
    for d in range(1, groups):
        pl.semaphore_signal(
            barrier, 1, device_id={"head": lax.rem(group + d, groups)}, device_id_type=MESH
        )

    @pl.when(has_next)
    def _():
        pl.semaphore_signal(barrier, 1, device_id={"seq": slab + 2}, device_id_type=MESH)

    @pl.when(place > 0)
    def _():
        pl.semaphore_signal(barrier, 1, device_id={"seq": slab - 2}, device_id_type=MESH)

    @pl.when(has_far)
    def _():
        pl.semaphore_signal(
            barrier, 1, device_id={"seq": slab + 2 * jump}, device_id_type=MESH
        )

    @pl.when(place >= jump)
    def _():
        pl.semaphore_signal(
            barrier, 1, device_id={"seq": slab - 2 * jump}, device_id_type=MESH
        )

    pl.semaphore_wait(
        barrier,
        groups
        + has_next.astype(jnp.int32)
        + (place > 0).astype(jnp.int32)
        + has_far.astype(jnp.int32)
        + (place >= jump).astype(jnp.int32),
    )
    def start_cross(t, kv, c, packed):
        for sender in range(2):
            runs = cross_runs(t, sender, sender)
            if runs is not None and (t == pack_at and cross_far(t, sender)) == packed:

                @pl.when(runs)
                def _():
                    cross(t, kv, c, sender).start()

    def chain_runs(t):
        if t == pack_at:
            return has_far
        return (place >= t) & has_next

    def chain_of(t, kv, c):
        return direct(kv, c) if t == pack_at else chain(t, kv, c)

    def start_chain(t, kv, c):
        if t < chain_len - 1 and t != pack_at:

            @pl.when(chain_runs(t))
            def _():
                chain(t, kv, c).start()

    def arrive(t, kv, c):
        @pl.when(place >= t)
        def _():
            chain_in(t, kv, c).wait_recv()

    def pack_arrived(kv):
        t = pack_at

        @pl.when(place >= t)
        def _():
            first = pl.multiple_of(((place - t) * 2 + side) * blocks, blocks)
            move = pltpu.make_async_copy(
                bufs[kv].at[pl.ds(first, blocks)], held.at[kv], held_sem.at[kv]
            )
            move.start()
            move.wait()
            for k in range(CAP):
                packed[kv, k] = held[kv, pack_ref[k]]

        for each in range(PIECES):
            start_cross(t, kv, each, True)

    def pass_on(t, kv, c):
        arrive(t, kv, c)
        start_chain(t, kv, c)
        start_cross(t, kv, c, False)
        if t == pack_at and c == PIECES - 1:
            pack_arrived(kv)

    order = [t for t in range(1, chain_len) if t != pack_at]
    order.insert(min(2, len(order)), pack_at)

    def wait_cross(kv):
        for t in range(chain_len):
            for c in range(PIECES):
                for sender in range(2):
                    runs = cross_runs(t, sender, 1 - sender)
                    if runs is not None:

                        @pl.when(runs)
                        def _():
                            cross(t, kv, c, sender).wait_recv()

    base = slab * blocks
    slashes, verticals = slash_ref.shape[1], vertical_ref.shape[1]

    low = blocks.bit_length() - 1

    def names(head, words):
        for n in range(verticals):
            block = vertical_ref[head, n]
            bit = jnp.int32(1) << (block & 31)
            words = tuple(
                word | jnp.where((block >> 5) == w, bit, 0) for w, word in enumerate(words)
            )
        offsets = jnp.int32(0)
        for n in range(slashes):
            offsets = offsets | (jnp.int32(1) << slash_ref[head, n])
        offsets_ref[head] = offsets
        return words

    def place_verticals(head, carry):
        for n in range(verticals):
            block = vertical_ref[head, n]
            first = (block >> low) << low
            in_slab = named_ref[block >> 5] >> (first & 31)
            below = in_slab & ((jnp.int32(1) << (block - first)) - 1)
            rank = jnp.int32(0)
            for u in range(blocks - 1):
                rank = rank + ((below >> u) & 1)
            found = jnp.where(
                block >= (slab - reach) * blocks, block, whole_blocks + (block >> low) * CAP + rank
            )
            found_ref[head * verticals + n] = jnp.where(block < base + blocks, found, base)
        return carry

    def list_pack(to_ref, of_slab):
        first = of_slab * blocks
        in_slab = named_ref[first >> 5] >> (first & 31)
        at = [jnp.int32(0) for _ in range(CAP)]
        count = jnp.int32(0)
        for n in range(blocks):
            hit = (in_slab >> n) & 1
            at = [x + jnp.where((hit == 1) & (count == k), n, 0) for k, x in enumerate(at)]
            count = count + hit
        for k in range(CAP):
            to_ref[k] = at[k]

    second = group % 2
    partner = group + 1 - 2 * second
    loads[0].wait()
    for c in range(PIECES):
        start_chain(0, 0, c)
        start_cross(0, 0, c, False)

    words = tuple(jnp.int32(0) for _ in range((whole_blocks + 31) // 32))
    for w, word in enumerate(lax.fori_loop(0, heads, names, words)):
        named_ref[w] = word
    list_pack(own_pack_ref, slab)
    loads[3].wait()
    loads[1].wait()

    start_direct(0)
    list_pack(pack_ref, jnp.maximum((place - pack_at) * 2 + side, 0))
    for t in order:
        for c in range(PIECES):
            pass_on(t, 0, c)
        if t == 1:
            lax.fori_loop(0, heads, place_verticals, 0)
            for n in range(blocks):
                v_buf[own_first + n] = held[1, n].T
    def send_values():
        for c in range(PIECES):
            start_chain(0, 1, c)
            start_cross(0, 1, c, False)
        start_direct(1)

    early_sent = min(2, chain_len - 1)

    def give_turn():
        for t in range(early_sent):
            for c in range(PIECES):

                @pl.when(chain_runs(t))
                def _():
                    chain_of(t, 1, c).wait_send()

        pl.semaphore_signal(turn_sem, 1, device_id={"head": partner}, device_id_type=MESH)

    def take_turn():
        pl.semaphore_wait(turn_sem, 1)
        send_values()

    pl.when(second == 0)(send_values)
    wait_cross(0)
    loads[2].wait()

    factor = math.log2(math.e) / math.sqrt(width)
    causal = lax.broadcasted_iota(jnp.int32, (BLK, BLK), 0) <= lax.broadcasted_iota(
        jnp.int32, (BLK, BLK), 1
    )
    share = blocks // groups
    share_rows = share * BLK

    def out_columns(group_of, head):
        return pl.ds(pl.multiple_of((group_of * heads + head) * width, width), width)

    def owner_of(r):
        return (group // 2 + r // 2 + 1) % (groups // 2) * 2 + (group + r + 1) % 2

    def sender_of(r):
        return (group // 2 + groups // 2 - 1 - r // 2) % (groups // 2) * 2 + (group + r + 1) % 2

    def out_copy(head, r):
        owner = owner_of(r)
        return pltpu.make_async_remote_copy(
            staged.at[head, pl.ds(pl.multiple_of(owner * share_rows, share_rows), share_rows)],
            out_ref.at[:, out_columns(group, head)],
            out_send.at[head, r], out_recv.at[head, r],
            device_id={"head": owner}, device_id_type=MESH,
        )

    def out_in(head, r):
        sender = sender_of(r)
        return pltpu.make_async_remote_copy(
            staged.at[head, pl.ds(0, share_rows)],
            out_ref.at[:, out_columns(sender, head)],
            out_send.at[head, r], out_recv.at[head, r],
            device_id={"head": sender}, device_id_type=MESH,
        )

    def out_own(head):
        return pltpu.make_async_copy(
            staged.at[head, pl.ds(pl.multiple_of(group * share_rows, share_rows), share_rows)],
            out_ref.at[:, out_columns(group, head)],
            out_local.at[head],
        )

    listed = 1 + slashes + verticals
    pairs = heads * blocks // 2 // rounds
    pairs_of_share = share // 2
    chunk_count = slashes // 2 + 1
    def relays(ts):
        return [functools.partial(pass_on, t, 1, c) for t in ts for c in range(PIECES)]

    first_relays = relays(order[:1])
    later_relays = relays(order[1:-1])
    last_relays = relays(order[-1:])
    if len(order) < 2:
        later_relays, last_relays = [], []
    events = [(FIRST_STEPS[0], 0, first_relays[:1]), (FIRST_STEPS[1], 0, first_relays[1:])]
    events += [(FIRST_STEPS[2], 0, [give_turn, *later_relays])]
    events += [(FIRST_STEPS[3], 0, last_relays)]
    events += [(SECOND_STEPS[0], 1, [take_turn])]
    events += [(SECOND_STEPS[1], 1, first_relays + later_relays + last_relays)]

    for q in range(blocks // 2):
        block_ref[q] = owner_of(q // pairs_of_share) * share + q % pairs_of_share * 2

    def pair_of(pair):
        q = lax.div(pair, heads)
        return lax.rem(pair, heads), q, block_ref[q]

    def reached(head, own, n):
        return own - slash_ref[head, n - 1]

    def listed_pair(buf, head, i, n):
        if n == 0:
            return buf[base + i], buf[base + i + 1]
        if n <= slashes:
            both = [reached(head, base + i + half, n) for half in range(2)]
            return [buf[jnp.where(x >= 0, x, base + i + half)] for half, x in enumerate(both)]
        shared = buf[found_ref[head * verticals + n - 1 - slashes]]
        return shared, shared

    def bias_of(head, i, n, half):
        own = base + i + half
        if n <= slashes:
            return jnp.where(reached(head, own, n) >= 0, 0.0, NEG)
        back = own - vertical_ref[head, n - 1 - slashes]
        covered = (offsets_ref[head] >> jnp.clip(back, 0, 31)) & 1
        return jnp.where((back > 0) & (covered == 0), 0.0, NEG)

    chunks = []
    for c in range(chunk_count):
        near = [0] if c == 0 else [2 * c - 1, 2 * c]
        chunks.append((near, [1 + slashes + n for n in range(2 * c, min(2 * c + 2, verticals))]))

    def weigh_round(first, *accs):
        ring = (accs[:RING], accs[RING:])
        buffers = (
            (scores_even, top_even, bias_even), (scores_odd, top_odd, bias_odd)
        )

        def members(c):
            for j in range(2):
                for m in range(2):
                    if j < len(chunks[c][m]):
                        slot = 2 * c + j if m else max(2 * c - 1, 0) + j
                        yield m, chunks[c][m][j], ring[m][slot if slot < RING else 1]

        def stage(head, i):
            columns = pl.ds(pl.multiple_of(head * width, width), width)
            both = [
                q_ref[pl.ds(pl.multiple_of((i + u) * BLK, BLK), BLK), columns] for u in range(2)
            ]
            pltpu.matmul_push_rhs(on_diagonal(*both), 0, 0, transpose=True)
            scaled = []
            for q in both:
                exact = q.astype(jnp.float32) * factor
                high = exact.astype(jnp.bfloat16)
                scaled.append(beside(high, (exact - high.astype(jnp.float32)).astype(jnp.bfloat16)))
            pltpu.matmul_push_rhs(stacked(*scaled), 0, 1, transpose=True)

        def score(head, i, c):
            fresh = [c == 0, c == 0]
            for m, n, acc in members(c):
                pltpu.matmul_acc_lhs(
                    acc, beside(*listed_pair(k_buf, head, i, n)), load_staged_rhs=0 if fresh[m] else None
                )
                fresh[m] = False

        def take(head, i, c, scores, top, biases):
            tops = [None, None]
            for m, n, acc in members(c):
                both = pltpu.matmul_pop(acc)
                for half in range(2):
                    x = both[:, half_columns(half)]
                    if n == 0:
                        x = jnp.where(causal, x, NEG)
                    scores[n * BLK : (n + 1) * BLK, half_columns(half)] = x
                    x = jnp.max(x.reshape(BLK // 8, 8, BLK), axis=0)
                    if n > 0:
                        bias = bias_of(head, i, n, half)
                        biases[2 * n + half] = bias
                        x = x + bias
                    if m == 0:
                        x = x * factor
                    tops[half] = x if tops[half] is None else jnp.maximum(tops[half], x)
                    yield
            for half in range(2):
                x = tops[half]
                if c > 0:
                    x = jnp.maximum(x, top[:, half_columns(half)])
                if c == chunk_count - 1:
                    x = jnp.broadcast_to(jnp.max(x, axis=0, keepdims=True), (8, BLK))
                top[:, half_columns(half)] = x

        def weigh(slot, c, scores, top, biases):
            for m, n, _ in members(c):
                for half in range(2):
                    x = scores[n * BLK : (n + 1) * BLK, half_columns(half)]
                    shift = top[0:1, half_columns(half)]
                    if n > 0:
                        shift = shift - biases[2 * n + half]
                    if m == 0:
                        x = x * factor
                    weights[slot, half, n * BLK : (n + 1) * BLK, :] = jnp.exp2(
                        x - shift
                    ).astype(jnp.bfloat16)
                    yield

        def drain(*steps):
            for step in steps:
                for _ in step:
                    pass

        def alternate(a, b):
            for _ in itertools.zip_longest(a, b):
                pass

        def advance(head, q):
            wraps = head + 1 == heads
            q = jnp.minimum(q + wraps.astype(jnp.int32), blocks // 2 - 1)
            return jnp.where(wraps, 0, head + 1), q, block_ref[q]

        def one_pair(step, parity, head, q, i, last_head, last_i):
            last, older = jnp.maximum(step - 1, 0), jnp.maximum(step - 2, 0)
            mine, other = buffers[parity], buffers[1 - parity]
            next_head, next_q, next_i = advance(head, q)

            def part(c):
                if c == 1:
                    alternate(
                        weigh(older, chunk_count - 1, *mine),
                        take(last_head, last_i, chunk_count - 1, *other),
                    )
                    score(head, i, 1)
                    return
                score(head, i, c)
                if c == 0:
                    alternate(
                        weigh(older, chunk_count - 2, *mine),
                        take(last_head, last_i, chunk_count - 2, *other),
                    )
                    return
                if c == chunk_count - 1:
                    stage(next_head, next_i)
                alternate(weigh(last, c - 2, *other), take(head, i, c - 2, *mine))

            for c in range(chunk_count):
                pl.when(slab > -1 - c // 2)(functools.partial(part, c))
            return next_head, next_q, next_i, head, i

        for m in range(2):
            for acc in ring[m]:
                pltpu.matmul_pop(acc)
        begin = pair_of(jnp.int32(first))
        stage(begin[0], begin[2])

        def two_pairs(step, carry):
            if first == 0:
                for at, of, acts in events:

                    @pl.when((step == min(at, pairs // 2 - 1)) & (second == of))
                    def _():
                        for act in acts:
                            act()

            carry = one_pair(2 * step, 0, *carry)
            return one_pair(2 * step + 1, 1, *carry)

        carry = lax.fori_loop(0, pairs // 2, two_pairs, (*begin, begin[0], begin[2]))
        for c in range(chunk_count - 2, chunk_count):
            drain(take(*carry[3:], c, *buffers[1]), weigh(pairs - 2, c, *buffers[0]))
        for c in range(chunk_count):
            drain(weigh(pairs - 1, c, *buffers[1]))
        for m in range(2):
            pltpu.matmul_acc_lhs(
                ring[m][0], jnp.zeros((BLK, 2 * BLK), jnp.bfloat16), load_staged_rhs=0
            )
            pltpu.matmul_pop(ring[m][0])

    def mix_round(first, *accs):
        ones = jnp.ones((16, 2 * BLK), jnp.bfloat16)

        def mix(pair, m, acc):
            head, _, i = pair_of(first + pair)
            slot = 0
            for n in range(1 + slashes):
                both = [weights[pair, half, n * BLK : (n + 1) * BLK, :] for half in range(2)]
                pltpu.matmul_push_rhs(on_diagonal(*both), slot, m)
                lhs = beside(*listed_pair(v_buf, head, i, n))
                pltpu.matmul_acc_lhs(acc, stacked(lhs, ones), load_staged_rhs=slot)
                slot = 1 - slot
                yield
            for n in range(1 + slashes, listed, 2):
                both = [weights[pair, half, n * BLK : (n + 2) * BLK, :] for half in range(2)]
                pltpu.matmul_push_rhs(beside(*both), slot, m)
                lhs = beside(*[listed_pair(v_buf, head, i, n + u)[0] for u in range(2)])
                pltpu.matmul_acc_lhs(acc, stacked(lhs, ones), load_staged_rhs=slot)
                slot = 1 - slot
                yield

        def some_pairs(step, carry):
            at = step * 2 * MIX_UNROLL
            for u in range(MIX_UNROLL):
                for _ in zip(
                    mix(at + 2 * u, 0, accs[u]), mix(at + 2 * u + 1, 1, accs[MIX_UNROLL + u])
                ):
                    pass
            for u in range(MIX_UNROLL):
                for m in range(2):
                    head, _, i = pair_of(first + at + 2 * u + m)
                    mixed = pltpu.matmul_pop(accs[m * MIX_UNROLL + u])
                    for half in range(2):
                        out = mixed[:width, half_columns(half)] / mixed[width : width + 1, half_columns(half)]
                        rows = pl.ds(pl.multiple_of((i + half) * BLK, BLK), BLK)
                        staged[head, rows, :] = out.T.astype(jnp.bfloat16)
            for u in range(2 * MIX_UNROLL):
                head, q, _ = pair_of(first + at + u)
                r = lax.div(q, pairs_of_share)
                whole = lax.rem(q, pairs_of_share) == pairs_of_share - 1

                @pl.when(whole & (r < groups - 1))
                def _():
                    out_copy(head, r).start()

                @pl.when(whole & (r == groups - 1))
                def _():
                    out_own(head).start()

            return carry

        for acc in accs:
            pltpu.matmul_pop(acc)
        lax.fori_loop(0, pairs // (2 * MIX_UNROLL), some_pairs, 0)

    for each in range(rounds):
        pl.run_scoped(
            functools.partial(weigh_round, each * pairs),
            *[pltpu.ACC(m)((BLK, 2 * BLK), jnp.float32) for m in range(2) for _ in range(RING)],
        )
        if each == 0:
            wait_cross(1)
        pl.run_scoped(
            functools.partial(mix_round, each * pairs),
            *[pltpu.ACC(m)((width + 16, 2 * BLK), jnp.float32) for m in range(2) for _ in range(MIX_UNROLL)],
        )

    for kv in range(2):
        for t in range(chain_len):
            for c in range(PIECES):
                if t < chain_len - 1:

                    runs = chain_runs(t)
                    if kv == 1 and t < early_sent:
                        runs = runs & (second == 1)

                    @pl.when(runs)
                    def _():
                        chain_of(t, kv, c).wait_send()

                for sender in range(2):
                    runs = cross_runs(t, sender, sender)
                    if runs is not None:

                        @pl.when(runs)
                        def _():
                            cross(t, kv, c, sender).wait_send()

    def finish(head, carry):
        out_own(head).wait()
        for r in range(groups - 1):
            out_copy(head, r).wait_send()
            out_in(head, r).wait_recv()
        return carry

    lax.fori_loop(0, heads, finish, 0)


def shards(queries, keys, values, vertical, slash):
    width = keys.shape[1]
    rows = queries.shape[0]
    blocks = rows // BLK
    heads = vertical.shape[0]
    slabs, groups = lax.axis_size("seq"), lax.axis_size("head")
    k = keys.reshape(blocks, BLK, width)
    v = values.reshape(blocks, BLK, width)
    slashes, verticals = slash.shape[1], vertical.shape[1]
    listed = 1 + slashes + verticals
    pairs = heads * blocks // 2
    room = VMEM_BYTES - 4 * (2 * BLK * width * slabs * (blocks + CAP) // 2)
    room -= 4 * rows * heads * width + 2 * 4 * listed * BLK * 2 * BLK + SPARE_BYTES
    rounds = ROUNDS
    while pairs // rounds * listed * BLK * 2 * BLK * 2 > room:
        rounds *= 2
    dma = pltpu.SemaphoreType.DMA
    hops = (slabs // 2, 2, PIECES)
    smem, anywhere = pl.BlockSpec(memory_space=pltpu.SMEM), pl.BlockSpec(memory_space=pl.ANY)
    return pl.pallas_call(
        functools.partial(
            layer_kernel,
            blocks=blocks,
            rounds=rounds,
            width=width,
            heads=heads,
            slabs=slabs,
            groups=groups,
        ),
        in_specs=[smem, smem, anywhere, anywhere, anywhere],
        out_specs=anywhere,
        out_shape=jax.ShapeDtypeStruct((rows // groups, groups * heads * width), jnp.bfloat16),
        scratch_shapes=[
            pltpu.SMEM(((slabs * blocks + 31) // 32,), jnp.int32),
            pltpu.SMEM((heads,), jnp.int32),
            pltpu.SMEM((vertical.size,), jnp.int32),
            pltpu.SMEM((CAP,), jnp.int32),
            pltpu.SMEM((CAP,), jnp.int32),
            pltpu.SMEM((blocks // 2,), jnp.int32),
            pltpu.SMEM((2 * listed,), jnp.float32),
            pltpu.SMEM((2 * listed,), jnp.float32),
            pltpu.VMEM(queries.shape, jnp.bfloat16),
            pltpu.VMEM((slabs * (blocks + CAP), BLK, width), jnp.bfloat16),
            pltpu.VMEM((slabs * (blocks + CAP), width, BLK), jnp.bfloat16),
            pltpu.VMEM((heads, rows, width), jnp.bfloat16),
            pltpu.VMEM((pairs // rounds, 2, listed * BLK, BLK), jnp.bfloat16),
            pltpu.VMEM((listed * BLK, 2 * BLK), jnp.float32),
            pltpu.VMEM((listed * BLK, 2 * BLK), jnp.float32),
            pltpu.VMEM((8, 2 * BLK), jnp.float32),
            pltpu.VMEM((8, 2 * BLK), jnp.float32),
            pltpu.VMEM((2, blocks, BLK, width), jnp.bfloat16),
            pltpu.VMEM((2, CAP, BLK, width), jnp.bfloat16),
            pltpu.VMEM((2, CAP, BLK, width), jnp.bfloat16),
            pltpu.SemaphoreType.REGULAR,
            dma((2,)),
            dma((4,)),
            dma(hops),
            dma(hops),
            dma(hops),
            dma(hops),
            dma((heads,)),
            dma((heads, groups - 1)),
            dma((heads, groups - 1)),
        ],
        compiler_params=pltpu.CompilerParams(
            collective_id=0, has_side_effects=True, vmem_limit_bytes=VMEM_BYTES
        ),
    )(slash, vertical, queries, k, v)


def solution(mesh):
    in_specs = (
        P("seq", "head"),
        P("seq", "head"),
        P("seq", "head"),
        P("head", None),
        P("head", None),
    )
    out_specs = P(("seq", "head"), None)
    return jax.shard_map(shards, mesh=mesh, in_specs=in_specs, out_specs=out_specs, check_vma=False)
```
